32 devices in a mesh: cuts: 8 (over z, x), mode: 4 (over y, core).
Axes of the slice: x: 2, y: 2, z: 4, core: 2. Of those that a mesh axis runs over, the one named last changes fastest.
Arguments:
- sliced_state: bfloat16 [8, 16, 4, 128, 2, 128], P(None, 'cuts', None, 'mode'), may hold values from -0.75 to 0.75
- gate_blocks: bfloat16 [32, 2, 128, 128], P('cuts'), may hold values from -0.375 to 0.375
- gate_slot: int32 [32], replicated, may hold values from 0 to 31, each once
- samples: int32 [8, 4096], replicated, may hold values from 0 to 65535
Outputs:
- amplitudes: float32 [32, 128, 2, 128], P('cuts', 'mode')
- sample_probs: float32 [8, 4096], replicated
- xeb_score: float32 [8], replicated
The draws below stay inside these ranges and needn't reach their ends.
Inputs may be any that keep to these rules, and one draw needn't show every extreme that they name: `gate_slot`: a permutation: every gate block has its own row of gate_blocks. `samples`: flat index s * 128 * 128 + p * 128 + q.
All inputs are finite; a program needn't handle non-finite values.
Results may differ from the reference program's by a relative error of at most 0.022.
Values may be sent and summed in bfloat16 or wider, within the bound.
A program may use at most 64 MiB of HBM per device.

```python
import jax
import jax.numpy as jnp

G = 128
S = 4
CIRC = 8
LAYERS = 2
SAMPLES = 4096
SLICES = 16
NBLK = 32


def plant(entries, rng, smallest, high):
    longest = entries.shape.index(max(entries.shape))
    spots = []
    for shift in (0, 1):
        where = [jax.random.randint(jax.random.fold_in(rng, axis), (), 0, length) for axis, length in enumerate(entries.shape)]
        where[longest] = (where[longest] + shift) % entries.shape[longest]
        spots.append(tuple(where))
    return entries.at[spots[0]].set(smallest).at[spots[1]].set(high)


def steps_of(own_key, extent, shards, smallest, high):
    level, own = 1.0, jax.random.fold_in(own_key, 6)
    for position, blocks in shards:
        steps = jnp.exp(jax.random.uniform(jax.random.fold_in(own, position), (blocks,), jnp.float32, smallest / len(shards), high / len(shards)))
        level = level * jnp.repeat(steps, extent[position] // blocks).reshape([-1 if axis == position else 1 for axis in range(len(extent))])
    return level


def bell_draw(stream_key, dims, deviation, most, split=(), held_as=jnp.bfloat16):
    level = steps_of(stream_key, dims, split, -0.22, 0.18) if split else 1.0
    array = jax.random.normal(stream_key, dims, jnp.float32) * deviation * level
    return jnp.minimum(jnp.maximum(array, -most), most).astype(held_as)


def setup_inputs(seed: int = 0) -> dict:
    arg_keys = jax.random.split(jax.random.key(seed), 5)
    return {
        "sliced_state": bell_draw(arg_keys[0], (CIRC, SLICES, S, G, 2, G), 0.125, 0.75, ((1, 8), (3, 4))),
        "gate_blocks": bell_draw(arg_keys[1], (NBLK, 2, G, G), (2 * G) ** -0.5, 0.375, ((0, 8),)),
        "gate_slot": jax.random.permutation(arg_keys[2], NBLK).astype(jnp.int32),
        "samples": plant(jax.random.randint(arg_keys[3], (CIRC, SAMPLES), 0, S * G * G), jax.random.fold_in(arg_keys[3], 1), 0, (S * G * G) - 1).astype(jnp.int32),
    }


def apply_gates(tensor, blocks):
    real_part = blocks[:, 0]
    imag_part = blocks[:, 1]
    stacked = jnp.concatenate([jnp.concatenate([real_part, imag_part], axis=2), jnp.concatenate([-imag_part, real_part], axis=2)], axis=1)
    layout = tensor.shape
    flattened = tensor.reshape(layout[0], -1, 2 * layout[-1])
    product = jnp.einsum("crk,ckn->crn", flattened.astype(jnp.float32), stacked.astype(jnp.float32))
    return product.astype(jnp.bfloat16).reshape(layout)


def reference(sliced_state, gate_blocks, gate_slot, samples):
    tensor = sliced_state
    circuit_ids = jnp.arange(CIRC, dtype=jnp.int32)
    for layer_index in range(LAYERS):
        for gate_kind in range(2):
            block_ids = (circuit_ids * LAYERS + layer_index) * 2 + gate_kind
            blocks = gate_blocks[gate_slot[block_ids]]
            if gate_kind == 1:
                tensor = jnp.swapaxes(tensor, 3, 5)
            tensor = apply_gates(tensor, blocks)
            if gate_kind == 1:
                tensor = jnp.swapaxes(tensor, 3, 5)
    amplitudes = jnp.sum(tensor.astype(jnp.float32), axis=1).reshape(CIRC * S, G, 2, G)
    magnitude = amplitudes[:, :, 0, :] ** 2 + amplitudes[:, :, 1, :] ** 2
    per_circuit = magnitude.reshape(CIRC, S * G * G)
    norm_total = jnp.sum(per_circuit, axis=1)
    picked = jnp.take_along_axis(per_circuit, samples, axis=1)
    sample_probs = picked * float(S * G * G) / norm_total[:, None]
    xeb_score = jnp.mean(sample_probs, axis=1)
    return amplitudes, sample_probs, xeb_score
```

```python
import functools

import jax
import jax.numpy as jnp
from jax import lax
from jax.experimental import pallas as pl
from jax.experimental.pallas import tpu as pltpu
from jax.sharding import PartitionSpec as P

MESH = pl.DeviceIdType.MESH
BF16 = jnp.bfloat16
F32 = jnp.float32


def dot(a, b):
    return jnp.dot(a, b, preferred_element_type=F32)


def stacked(real_part, imag_part):
    top = jnp.concatenate([real_part, imag_part], axis=1)
    bottom = jnp.concatenate([-imag_part, real_part], axis=1)
    return jnp.concatenate([top, bottom], axis=0)


def kernel(
    cfg,
    x_ref,
    gates_ref,
    samples_ref,
    slot_ref,
    amp_ref,
    probs_ref,
    xeb_ref,
    part,
    got,
    mine,
    whole,
    relay,
    pick,
    blocks,
    plane,
    own,
    land,
    gate_send,
    gate_recv,
    pick_send,
    pick_recv,
    part_send,
    part_recv,
    mode_send,
    mode_recv,
    prob_send,
    prob_recv,
):
    ncuts, nmode, circuits, spect, width, per_circuit = cfg
    ndev = ncuts * nmode
    k = lax.axis_index("cuts")
    m = lax.axis_index("mode")
    me = k * nmode + m
    sharers = ncuts // circuits
    c = k // sharers
    held = gates_ref.shape[0]
    npieces, _, piece = blocks.shape[0], blocks.shape[1], blocks.shape[2]
    rows_out = amp_ref.shape[0]
    pb2 = amp_ref.shape[1]
    ns = own.shape[1]

    barrier = pltpu.get_barrier_semaphore()

    @pl.loop(1, ndev)
    def _(i):
        d = lax.rem(me + i, ndev)
        pl.semaphore_signal(
            barrier, inc=1, device_id=(d // nmode, lax.rem(d, nmode)), device_id_type=MESH
        )

    for i in range(circuits):
        total = x_ref[i, 0].astype(F32)
        for j in range(1, x_ref.shape[1]):
            total = total + x_ref[i, j].astype(F32)
        part[i] = total.astype(BF16)

    pl.semaphore_wait(barrier, ndev - 1)

    def gate_copy(src, dst):
        rows = pl.ds(pl.multiple_of(dst * piece, piece), piece)
        return pltpu.make_async_remote_copy(
            src_ref=gates_ref.at[:, rows],
            dst_ref=relay.at[pl.ds(src * held, held)],
            send_sem=gate_send.at[dst],
            recv_sem=gate_recv.at[src],
            device_id=(dst, m),
            device_id_type=MESH,
        )

    def pick_copy(src, dst):
        return pltpu.make_async_remote_copy(
            src_ref=pick.at[dst // sharers],
            dst_ref=blocks.at[src],
            send_sem=pick_send.at[dst],
            recv_sem=pick_recv.at[src],
            device_id=(dst, m),
            device_id_type=MESH,
        )

    def part_copy(src, dst):
        return pltpu.make_async_remote_copy(
            src_ref=part.at[dst // sharers],
            dst_ref=got.at[src],
            send_sem=part_send.at[dst],
            recv_sem=part_recv.at[src],
            device_id=(dst, m),
            device_id_type=MESH,
        )

    def mode_copy(src, dst):
        return pltpu.make_async_remote_copy(
            src_ref=mine,
            dst_ref=whole.at[src],
            send_sem=mode_send.at[dst],
            recv_sem=mode_recv.at[src],
            device_id=(k, dst),
            device_id_type=MESH,
        )

    def prob_copy(src, dst):
        return pltpu.make_async_remote_copy(
            src_ref=own,
            dst_ref=land.at[src],
            send_sem=prob_send.at[dst],
            recv_sem=prob_recv.at[src],
            device_id=(dst // nmode, lax.rem(dst, nmode)),
            device_id_type=MESH,
        )

    def relays(action):
        if npieces == ncuts:
            action()
        else:
            pl.when(k < npieces)(action)

    for i in range(1, ncuts):
        j = lax.rem(k + i, ncuts)

        def start_gate():
            gate_copy(k, j).start()

        if npieces == ncuts:
            start_gate()
        else:
            pl.when(j < npieces)(start_gate)
    for i in range(1, ncuts):
        part_copy(k, lax.rem(k + i, ncuts)).start()

    def relay_gates():
        rows = pl.ds(pl.multiple_of(k * piece, piece), piece)
        relay[pl.ds(k * held, held)] = gates_ref[:, rows]
        for i in range(1, ncuts):
            gate_copy(lax.rem(k + ncuts - i, ncuts), k).wait_recv()
        for i in range(circuits):
            for b in range(per_circuit):
                pick[i, b] = relay[slot_ref[i * per_circuit + b]]
        for i in range(1, ncuts):
            pick_copy(k, lax.rem(k + i, ncuts)).start()
        blocks[k] = pick[c]

    relays(relay_gates)

    total = part[c].astype(F32)
    for i in range(1, ncuts):
        j = lax.rem(k + ncuts - i, ncuts)
        part_copy(j, k).wait_recv()
        total = total + got[j].astype(F32)
    mine[...] = total.astype(BF16)
    for i in range(1, nmode):
        mode_copy(m, lax.rem(m + i, nmode)).start()
    whole[m] = total.astype(BF16)

    for i in range(1, ncuts):
        j = lax.rem(k + ncuts - i, ncuts)

        def wait_pick():
            pick_copy(j, k).wait_recv()

        if npieces == ncuts:
            wait_pick()
        else:
            pl.when(j < npieces)(wait_pick)

    def block(b):
        return blocks[:, b].reshape(2 * width, width)

    def composed(kind):
        left = None
        for b in range(kind, per_circuit, 2):
            gate = block(b)
            real_part, imag_part = gate[:width], gate[width:]
            if left is None:
                left = jnp.concatenate([real_part, imag_part], axis=1)
            else:
                left = dot(left, stacked(real_part, imag_part)).astype(BF16)
        return left[:, :width], left[:, width:]

    right = stacked(*composed(0))
    col_real, col_imag = composed(1)
    left_t = stacked(col_real, col_imag).astype(F32).T.astype(BF16)

    for i in range(1, nmode):
        mode_copy(lax.rem(m + nmode - i, nmode), m).wait_recv()

    for s in range(spect):
        for j in range(nmode):
            plane[s, j * pb2 : (j + 1) * pb2] = whole[j, s * pb2 : (s + 1) * pb2].astype(F32)
    state = jnp.concatenate(
        [
            jnp.concatenate(
                [plane[s, pl.ds(0, width, stride=2), :], plane[s, pl.ds(1, width, stride=2), :]],
                axis=1,
            )
            for s in range(spect)
        ],
        axis=0,
    ).astype(BF16)
    state = dot(state, right).astype(BF16)
    state = jnp.concatenate(
        [
            jnp.concatenate(
                [
                    state[s * width : (s + 1) * width, r * width : (r + 1) * width]
                    for s in range(spect)
                ],
                axis=1,
            )
            for r in range(2)
        ],
        axis=0,
    )
    out = dot(left_t, state)
    magnitude = out[:width] * out[:width] + out[width:] * out[width:]
    norm = jnp.sum(jnp.sum(magnitude, axis=0, keepdims=True), axis=1, keepdims=True)

    table = jnp.concatenate(
        [magnitude[:, s * width : (s + 1) * width] for s in range(spect)], axis=0
    )
    high = table.astype(BF16)
    low = (table - high.astype(F32)).astype(BF16)
    table_t = jnp.concatenate([high, low], axis=1)
    group = lax.rem(k, sharers) * nmode + m
    chunk = samples_ref[:, pl.ds(pl.multiple_of(group * ns, ns), ns)]
    ours = lax.broadcasted_iota(jnp.int32, chunk.shape, 0) == c
    wanted = jnp.sum(jnp.where(ours, chunk, 0), axis=0, keepdims=True)
    row_id = wanted // width
    col_id = wanted - row_id * width
    row_hot = (
        (lax.broadcasted_iota(jnp.int32, (spect * width, ns), 0) == row_id)
        .astype(F32)
        .astype(BF16)
    )
    found = lax.dot_general(
        table_t, row_hot, (((0,), (0,)), ((), ())), preferred_element_type=F32
    )
    found = found[:width] + found[width:]
    col_hot = lax.broadcasted_iota(jnp.int32, (width, ns), 0) == col_id
    mass = jnp.sum(jnp.where(col_hot, found, 0.0), axis=0, keepdims=True)
    prob = mass * float(spect * width * width) / norm
    own[...] = prob
    land[me] = prob

    @pl.loop(1, ndev)
    def _(i):
        prob_copy(me, lax.rem(me + i, ndev)).start()

    for s in range(spect):
        for r in range(2):
            plane[s, pl.ds(r, width, stride=2), :] = out[
                r * width : (r + 1) * width, s * width : (s + 1) * width
            ]
    first = lax.rem(k, sharers) * rows_out
    amp_ref[...] = plane[pl.ds(first, rows_out), pl.ds(pl.multiple_of(m * pb2, pb2), pb2), :]

    for i in range(1, ncuts):
        j = lax.rem(k + i, ncuts)

        def end_gate():
            gate_copy(k, j).wait_send()

        if npieces == ncuts:
            end_gate()
        else:
            pl.when(j < npieces)(end_gate)

        def end_pick():
            pick_copy(k, j).wait_send()

        relays(end_pick)
        part_copy(k, j).wait_send()
    for i in range(1, nmode):
        mode_copy(m, lax.rem(m + i, nmode)).wait_send()

    @pl.loop(1, ndev)
    def _(i):
        prob_copy(me, lax.rem(me + i, ndev)).wait_send()
        prob_copy(lax.rem(me + ndev - i, ndev), me).wait_recv()

    for d in range(ndev):
        dk, dm = d // nmode, d % nmode
        dc = dk // sharers
        at = (dk % sharers * nmode + dm) * ns
        probs_ref[dc : dc + 1, at : at + ns] = land[d]
    xeb_ref[...] = jnp.broadcast_to(
        jnp.mean(probs_ref[...], axis=1, keepdims=True), xeb_ref.shape
    )


def on_device(mesh, sliced_state, gate_blocks, gate_slot, samples):
    ncuts, nmode = mesh.shape["cuts"], mesh.shape["mode"]
    ndev = ncuts * nmode
    circuits, local_slices, spect, pb, _, width = sliced_state.shape
    held = gate_blocks.shape[0]
    nblk = gate_slot.shape[0]
    per_circuit = nblk // circuits
    assert ncuts % circuits == 0
    sharers = ncuts // circuits
    assert spect % sharers == 0
    rows_out = spect // sharers
    nsamples = samples.shape[1]
    ns = nsamples // (sharers * nmode)
    npieces = min(ncuts, 2 * width // 16)
    piece = 2 * width // npieces
    rows = spect * pb * 2
    cfg = (ncuts, nmode, circuits, spect, width, per_circuit)
    vmem = pl.BlockSpec(memory_space=pltpu.VMEM)
    dma = pltpu.SemaphoreType.DMA
    amplitudes, probs, xeb = pl.pallas_call(
        functools.partial(kernel, cfg),
        out_shape=[
            jax.ShapeDtypeStruct((rows_out, pb * 2, width), F32),
            jax.ShapeDtypeStruct((circuits, nsamples), F32),
            jax.ShapeDtypeStruct((circuits, 128), F32),
        ],
        in_specs=[vmem, vmem, vmem, pl.BlockSpec(memory_space=pltpu.SMEM)],
        out_specs=[vmem, vmem, vmem],
        scratch_shapes=[
            pltpu.VMEM((circuits, rows, width), BF16),
            pltpu.VMEM((ncuts, rows, width), BF16),
            pltpu.VMEM((rows, width), BF16),
            pltpu.VMEM((nmode, rows, width), BF16),
            pltpu.VMEM((nblk, piece, width), BF16),
            pltpu.VMEM((circuits, per_circuit, piece, width), BF16),
            pltpu.VMEM((npieces, per_circuit, piece, width), BF16),
            pltpu.VMEM((spect, 2 * width, width), F32),
            pltpu.VMEM((1, ns), F32),
            pltpu.VMEM((ndev, 1, ns), F32),
            dma((ncuts,)),
            dma((ncuts,)),
            dma((ncuts,)),
            dma((ncuts,)),
            dma((ncuts,)),
            dma((ncuts,)),
            dma((nmode,)),
            dma((nmode,)),
            dma((ndev,)),
            dma((ndev,)),
        ],
        compiler_params=pltpu.CompilerParams(collective_id=0, has_side_effects=True),
    )(
        sliced_state.reshape(circuits, local_slices, rows, width),
        gate_blocks.reshape(held, 2 * width, width),
        samples,
        gate_slot,
    )
    return (amplitudes.reshape(rows_out, pb, 2, width), probs, xeb[:, 0])


def solution(mesh):
    in_specs = (P(None, "cuts", None, "mode", None, None), P("cuts", None, None, None), P(), P())
    out_specs = (P("cuts", "mode", None, None), P(), P())
    return jax.shard_map(
        functools.partial(on_device, mesh),
        mesh=mesh,
        in_specs=in_specs,
        out_specs=out_specs,
        check_vma=False,
    )
```
